32 devices in a mesh: pb: 4 (over z), ka: 8 (over y, x, core).
Axes of the slice: x: 2, y: 2, z: 4, core: 2. Of those that a mesh axis runs over, the one named last changes fastest.
Arguments:
- queries: float32 [1, 4096, 128], P(None, ('pb', 'ka')), may hold values from -6 to 6
- keys: float32 [1, 4096, 128], P(None, ('ka', 'pb')), may hold values from -6 to 6
- values: float32 [1, 4096, 128], P(None, ('ka', 'pb')), may hold values from -6 to 6
- tangent_q: float32 [1, 4096, 128], P(None, ('pb', 'ka')), may hold values from -6 to 6
- tangent_k: float32 [1, 4096, 128], P(None, ('ka', 'pb')), may hold values from -6 to 6
- tangent_v: float32 [1, 4096, 128], P(None, ('ka', 'pb')), may hold values from -6 to 6
Outputs:
- attended: float32 [1, 4096, 128], P(None, ('pb', 'ka'))
- attended_tangent: float32 [1, 4096, 128], P(None, ('pb', 'ka'))
The draws below stay inside these ranges and needn't reach their ends.
All inputs are finite; a program needn't handle non-finite values.
Results may differ from the reference program's by a relative error of at most 0.0003.
Values sent between devices are 32-bit elements; how exact they have to be, the bound alone decides.
No kernel may reach another device: no remote copies, remote signals or barrier semaphores. Data moves between devices by JAX's collectives and lax.ppermute only.
A program may use at most 128 MiB of HBM per device.

```python
import jax
import jax.numpy as jnp
from jax import lax

DH = 128
HEADS = 1
SEQ = 4096


def draw_queries(key, part):
    fresh = jax.random.fold_in(key, 1)
    return jnp.clip(jax.random.normal(fresh, (HEADS, SEQ, DH), jnp.float32), -6.0, 6.0)


def draw_keys(key, part):
    fresh = jax.random.fold_in(key, 2)
    return jnp.clip(jax.random.normal(fresh, (HEADS, SEQ, DH), jnp.float32), -6.0, 6.0)


def block_scale(own_key, shape, shards, least, largest):
    level, own = 1.0, jax.random.fold_in(own_key, 6)
    for axis_at, shards_of in shards:
        heights = jnp.exp(jax.random.uniform(jax.random.fold_in(own, axis_at), (shards_of,), jnp.float32, least / len(shards), largest / len(shards)))
        level = level * jnp.repeat(heights, shape[axis_at] // shards_of).reshape([-1 if axis == axis_at else 1 for axis in range(len(shape))])
    return level


def gaussian(rng, shape, spread, limit, shards=(), held_as=jnp.bfloat16):
    drawn = jax.random.normal(rng, shape, jnp.float32) * spread
    if len(shards) > 0:
        drawn = block_scale(rng, shape, shards, -0.22, 0.18) * drawn
    return jnp.clip(drawn, min=-limit, max=limit).astype(held_as)


def setup_inputs(seed: int = 0) -> dict:
    seeds = jax.random.split(jax.random.key(seed), 7)
    queries = draw_queries(jax.random.fold_in(seeds[6], 71), 0)
    keys = draw_keys(jax.random.fold_in(seeds[6], 71), 0)
    values = gaussian(seeds[2], (HEADS, SEQ, DH), 1.0, 6.0, ((1, 32),), jnp.float32)
    tangent_q = gaussian(seeds[3], (HEADS, SEQ, DH), 1.0, 6.0, ((1, 32),), jnp.float32)
    tangent_k = gaussian(seeds[4], (HEADS, SEQ, DH), 1.0, 6.0, ((1, 32),), jnp.float32)
    tangent_v = gaussian(seeds[5], (HEADS, SEQ, DH), 1.0, 6.0, ((1, 32),), jnp.float32)
    return dict(queries=queries, keys=keys, values=values, tangent_q=tangent_q, tangent_k=tangent_k, tangent_v=tangent_v)


def attend_block(query_blk, dquery_blk, head_keys, head_dkeys, head_values, head_dvalues):
    highest = lax.Precision.HIGHEST
    factor = DH ** -0.5
    scores = jnp.dot(query_blk, head_keys.T, precision=highest) * factor
    tangent = (jnp.dot(dquery_blk, head_keys.T, precision=highest) + jnp.dot(query_blk, head_dkeys.T, precision=highest)) * factor
    peak = jnp.max(scores, axis=1, keepdims=True)
    weights = jnp.exp(scores - peak)
    total = jnp.sum(weights, axis=1, keepdims=True)
    product = weights * tangent
    drift = jnp.sum(product, axis=1, keepdims=True) / total
    output = jnp.dot(weights, head_values, precision=highest) / total
    moved = (jnp.dot(weights, head_dvalues, precision=highest) + jnp.dot(product, head_values, precision=highest)) / total
    return output, moved - output * drift


def reference(queries, keys, values, tangent_q, tangent_k, tangent_v):
    block = min(1024, SEQ)
    count = SEQ // block

    def per_head(items):
        head_q, head_dq, head_k, head_dk, head_v, head_dv = items
        split_q = head_q.reshape(count, block, DH)
        split_dq = head_dq.reshape(count, block, DH)

        def per_block(pair):
            return attend_block(pair[0], pair[1], head_k, head_dk, head_v, head_dv)

        result = lax.map(per_block, (split_q, split_dq))
        return result[0].reshape(SEQ, DH), result[1].reshape(SEQ, DH)

    whole = lax.map(per_head, (queries, tangent_q, keys, tangent_k, values, tangent_v))
    return whole[0], whole[1]
```

```python
import functools

import jax
import jax.numpy as jnp
from jax import lax
from jax.experimental import pallas as pl
from jax.experimental.pallas import tpu as pltpu
from jax.sharding import PartitionSpec as P

F32 = jnp.float32
BF16 = jnp.bfloat16
VMEM = pl.BlockSpec(memory_space=pltpu.VMEM)
VMEM_LIMIT = 48 * 1024 * 1024


def split(x):
    high = x.astype(BF16)
    return high, (x - high.astype(F32)).astype(BF16)


def nt(a, b):
    return lax.dot_general(a, b, (((1,), (1,)), ((), ())), preferred_element_type=F32)


def nn(a, b):
    return jnp.dot(a, b, preferred_element_type=F32)


def attend_kernel(n_q, n_kv, has_state, last, *refs):
    q_refs, kv_refs = refs[:n_q], refs[n_q : n_q + n_kv]
    rest = refs[n_q + n_kv :]
    state_ref = None
    if has_state:
        state_ref, rest = rest[0], rest[1:]
    n_out = n_q if last else 1
    outs, (kk_s, kh_s, kl_s, vh_s, vl_s, vv_s) = rest[:n_out], rest[n_out:]
    rows, width = q_refs[0].shape[1:]
    keys = kv_refs[0].shape[1]
    factor = width ** (-0.5)
    for j, ref in enumerate(kv_refs):
        at = slice(j * keys, (j + 1) * keys)
        kh, kl = split(ref[0])
        dkh, dkl = split(ref[1])
        vh, vl = split(ref[2])
        dvh, dvl = split(ref[3])
        kk_s[at] = jnp.concatenate([kh, kh], axis=1)
        kh_s[at] = jnp.concatenate([kh, dkh], axis=1)
        kl_s[at] = jnp.concatenate([kl, dkl], axis=1)
        vh_s[at] = jnp.concatenate([vh, dvh], axis=1)
        vl_s[at] = jnp.concatenate([vl, dvl], axis=1)
        vv_s[at] = jnp.concatenate([vh, vl], axis=1)
    for i, ref in enumerate(q_refs):
        qh, ql = split(ref[0] * factor)
        dqh, dql = split(ref[1] * factor)
        high = jnp.concatenate([dqh, qh], axis=1)
        low = jnp.concatenate([dql, ql], axis=1)
        scores = nt(jnp.concatenate([qh, ql], axis=1), kk_s[...]) + nt(qh, kl_s[:, :width])
        tangent = nt(high, kh_s[...]) + nt(low, kh_s[...]) + nt(high, kl_s[...])
        peak = jnp.max(scores, axis=1, keepdims=True)
        at = slice(i * rows, (i + 1) * rows)
        if has_state:
            old = state_ref[0, at, :1]
            peak = jnp.maximum(peak, old)
            rescale = jnp.exp(old - peak)
        weights = jnp.exp(scores - peak)
        product = weights * tangent
        total = sum(weights[:, c : c + 128] for c in range(0, weights.shape[1], 128))
        drift = sum(product[:, c : c + 128] for c in range(0, product.shape[1], 128))
        wh, wl = split(weights)
        ph, plow = split(product)
        both = nn(wh, vh_s[...]) + nn(wl, vh_s[...]) + nn(wh, vl_s[...])
        extra = nn(ph, vv_s[...])
        numer = both[:, :width]
        tnumer = both[:, width:] + (extra[:, :width] + extra[:, width:] + nn(plow, vh_s[:, :width]))
        if has_state:
            total = total + state_ref[1, at] * rescale
            drift = drift + state_ref[2, at] * rescale
            numer = numer + state_ref[3, at] * rescale
            tnumer = tnumer + state_ref[4, at] * rescale
        if last:
            lane = lax.broadcasted_iota(jnp.int32, (rows, 128), 1)
            total = jnp.sum(total, axis=1, keepdims=True)
            drift = jnp.sum(drift, axis=1, keepdims=True)
            stats = jnp.where(lane == 0, peak, jnp.where(lane == 1, total, drift))
            outs[i][:rows] = numer
            outs[i][rows : 2 * rows] = tnumer
            outs[i][2 * rows :] = stats.T[:8]
        else:
            outs[0][0, at] = jnp.broadcast_to(peak, (rows, 128))
            outs[0][1, at] = total
            outs[0][2, at] = drift
            outs[0][3, at] = numer
            outs[0][4, at] = tnumer


def attend(q_blocks, kv_blocks, state, last):
    n_q, n_kv = len(q_blocks), len(kv_blocks)
    _, rows, width = q_blocks[0].shape
    keys = n_kv * kv_blocks[0].shape[1]
    if last:
        out_shape = [jax.ShapeDtypeStruct((2 * rows + 8, width), F32)] * n_q
    else:
        out_shape = [jax.ShapeDtypeStruct((5, n_q * rows, width), F32)]
    args = tuple(q_blocks) + tuple(kv_blocks) + (() if state is None else (state,))
    return pl.pallas_call(
        functools.partial(attend_kernel, n_q, n_kv, state is not None, last),
        out_shape=out_shape,
        in_specs=[VMEM] * len(args),
        out_specs=[VMEM] * len(out_shape),
        scratch_shapes=[pltpu.VMEM((keys, 2 * width), BF16)] * 6,
        compiler_params=pltpu.CompilerParams(vmem_limit_bytes=VMEM_LIMIT),
        cost_estimate=pl.CostEstimate(
            flops=40 * n_q * rows * keys * width, bytes_accessed=0, transcendentals=n_q * rows * keys
        ),
    )(*args)


def join_kernel(*refs):
    parts, (out_ref, tout_ref) = refs[:-2], refs[-2:]
    rows, width = out_ref.shape
    stats = []
    for ref in parts:
        spread = jnp.concatenate([ref[2 * rows :], jnp.zeros((rows - 8, width), F32)], axis=0).T
        stats.append((spread[:, 0:1], spread[:, 1:2], spread[:, 2:3]))
    peak = functools.reduce(jnp.maximum, [s[0] for s in stats])
    scale = [jnp.exp(s[0] - peak) for s in stats]
    total = sum(s[1] * e for s, e in zip(stats, scale))
    drift = sum(s[2] * e for s, e in zip(stats, scale))
    numer = sum(ref[:rows] * e for ref, e in zip(parts, scale))
    tnumer = sum(ref[rows : 2 * rows] * e for ref, e in zip(parts, scale))
    inverse = 1.0 / total
    attended = numer * inverse
    out_ref[...] = attended
    tout_ref[...] = tnumer * inverse - attended * (drift * inverse)


def join(parts):
    rows, width = (parts[0].shape[0] - 8) // 2, parts[0].shape[1]
    return pl.pallas_call(
        join_kernel,
        out_shape=[jax.ShapeDtypeStruct((rows, width), F32)] * 2,
        in_specs=[VMEM] * len(parts),
        out_specs=[VMEM] * 2,
        compiler_params=pltpu.CompilerParams(vmem_limit_bytes=VMEM_LIMIT),
    )(*parts)


def partner(i, d, n):
    return i ^ d if n & (n - 1) == 0 else (i + d) % n


def swap(x, axis, d, n, back=False):
    pairs = [(i, partner(i, d, n)) for i in range(n)]
    if back:
        pairs = [(b, a) for a, b in pairs]
    return lax.ppermute(x, axis, pairs)


def one_head(qq, kv, n_pb, n_ka):
    inner = 2 if n_ka % 2 == 0 else 1
    outer = n_ka // inner

    def across(x, d):
        pairs = [(i, partner(i // inner, d, outer) * inner + i % inner) for i in range(n_ka)]
        return lax.ppermute(x, "ka", pairs)

    def beside(x):
        return lax.ppermute(x, "ka", [(i, i ^ 1) for i in range(n_ka)])

    q_blocks = [qq] + [swap(qq, "pb", e, n_pb) for e in range(1, n_pb)]
    kv_blocks = [kv] + [across(kv, d) for d in range(1, outer)]
    if inner == 2:
        kv_blocks = [b for x in kv_blocks for b in (x, beside(x))]
    early = kv_blocks[:-inner]
    state = None
    if early:
        (state,) = attend(q_blocks, early, None, False)
    partials = attend(q_blocks, kv_blocks[len(early) :], state, True)
    parts = [partials[0]] + [swap(partials[e], "pb", e, n_pb, back=True) for e in range(1, n_pb)]
    return join(parts)


def solution(mesh):
    n_pb, n_ka = mesh.shape["pb"], mesh.shape["ka"]

    def body(queries, keys, values, tangent_q, tangent_k, tangent_v):
        outs = []
        for h in range(queries.shape[0]):
            one = slice(h, h + 1)
            qq = jnp.concatenate([queries[one], tangent_q[one]], axis=0)
            kv = jnp.concatenate([keys[one], tangent_k[one], values[one], tangent_v[one]], axis=0)
            outs.append(one_head(qq, kv, n_pb, n_ka))
        return tuple(jnp.stack([o[t] for o in outs]) for t in range(2))

    return jax.shard_map(
        body,
        mesh=mesh,
        in_specs=(
            P(None, ("pb", "ka"), None),
            P(None, ("ka", "pb"), None),
            P(None, ("ka", "pb"), None),
            P(None, ("pb", "ka"), None),
            P(None, ("ka", "pb"), None),
            P(None, ("ka", "pb"), None),
        ),
        out_specs=(P(None, ("pb", "ka"), None), P(None, ("pb", "ka"), None)),
        check_vma=False,
    )
```
